32 devices in a mesh: dp: 8 (over y, x, core), concept: 4 (over z).
Axes of the slice: x: 2, y: 2, z: 4, core: 2. Of those that a mesh axis runs over, the one named last changes fastest.
Arguments:
- text: bfloat16 [4096, 1024], P('dp', 'concept'), may hold values from -6 to 6
- concept_table: bfloat16 [24576, 1024], P('dp', 'concept'), may hold values from -6 to 6
- ids: int32 [4096], P('dp'), may hold values from 0 to 24575, as said below
Outputs:
- balanced: float32 [4096], P('dp')
The draws below stay inside these ranges and needn't reach their ends.
Inputs may be any that keep to these rules, and one draw needn't show every extreme that they name: In the 512 pairs of one index of dp, at most 128 ids fall in any one aligned range of 3072 concepts (c * 3072 to (c + 1) * 3072 - 1); in each such block of pairs some range holds exactly 128.
All inputs are finite; a program needn't handle non-finite values.
Results may differ from the reference program's by a relative error of at most 0.0003.
Values may be sent and summed in bfloat16 or wider, within the bound.
No kernel may reach another device: no remote copies, remote signals or barrier semaphores. Data moves between devices by JAX's collectives and lax.ppermute only.
A program may use at most 64 MiB of HBM per device.

```python
import jax
import jax.numpy as jnp
from jax import lax

D = 1024
CONC_OWN = 3072
PAIR_DEV = 512
CAP = 16
SLOT = 128
CONCEPTS = 24576
PAIRS = 4096
N_DP = 8


def draw_ids(key, part):
    keys = jax.random.split(jax.random.fold_in(key, 17), N_DP)

    def one_block(block_key):
        first, second, third, fourth = jax.random.split(block_key, 4)
        favoured = jax.random.randint(first, (), 0, N_DP)
        places = jax.random.permutation(second, N_DP * SLOT)
        holders = jnp.arange(N_DP * SLOT, dtype=jnp.int32) // SLOT
        scores = jnp.where(holders == favoured, places - N_DP * SLOT, places)
        order = jnp.argsort(scores, stable=True)
        owners = (order[:PAIR_DEV] // SLOT).astype(jnp.int32)
        owners = owners[jax.random.permutation(fourth, PAIR_DEV)]
        raw = jax.random.randint(third, (PAIR_DEV,), 0, CONC_OWN)
        squared = raw * raw // CONC_OWN
        cubed = squared * raw // CONC_OWN
        return (owners * CONC_OWN + cubed).astype(jnp.int32)
    return jax.vmap(one_block)(keys).reshape(-1)


def levels(rng, dims, cuts, smallest, high):
    def one(axis_at, shards_of):
        steps = jax.random.uniform(jax.random.fold_in(jax.random.fold_in(rng, 6), axis_at), (shards_of,), jnp.float32, smallest / len(cuts), high / len(cuts))
        return jnp.repeat(jnp.exp(steps), dims[axis_at] // shards_of).reshape((-1,) + (1,) * (len(dims) - axis_at - 1))

    loudness = one(*cuts[0])
    for cut in cuts[1:]:
        loudness = loudness * one(*cut)
    return loudness


def bell_draw(own_key, shape, width, bound, cuts=(), kind=jnp.bfloat16):
    array = width * jax.random.normal(own_key, shape, jnp.float32)
    if cuts:
        array = array * levels(own_key, shape, cuts, -0.22, 0.18)
    return jnp.clip(array, -bound, bound).astype(kind)


def setup_inputs(seed: int = 0) -> dict:
    splits = jax.random.split(jax.random.key(seed), 4)
    text = bell_draw(splits[0], (PAIRS, D), 1.0, 6.0, ((0, 8), (1, 4)))
    concept_table = bell_draw(splits[1], (CONCEPTS, D), 1.0, 6.0, ((0, 8), (1, 4)))
    ids = draw_ids(jax.random.fold_in(splits[3], 71), 0)
    return {"text": text, "concept_table": concept_table, "ids": ids}


logit_scale = 64.0
epsilon = 1e-06

def reference(text, concept_table, ids):
    text_blocks = text.reshape(N_DP, PAIR_DEV, D)
    id_blocks = ids.reshape(N_DP, PAIR_DEV)

    def one_block(args):
        block_text, block_ids = args
        pieces = jnp.take(concept_table, block_ids, axis=0).astype(jnp.float32)
        floats = block_text.astype(jnp.float32)
        return (lax.optimization_barrier(jnp.sum(floats * pieces, axis=1)), lax.optimization_barrier(jnp.sum(floats * floats, axis=1)), lax.optimization_barrier(jnp.sum(pieces * pieces, axis=1)))
    dot, tsq, csq = lax.map(one_block, (text_blocks, id_blocks))
    dot = dot.reshape(-1)
    tsq = tsq.reshape(-1)
    csq = csq.reshape(-1)
    match = jax.nn.sigmoid(logit_scale * dot * lax.rsqrt(tsq + epsilon) * lax.rsqrt(csq + epsilon))
    count = jnp.zeros((CONCEPTS,), jnp.float32).at[ids].add(match)
    capped = CAP * 1.0
    return match * capped / jnp.maximum(jnp.take(count, ids), capped)
```

```python
import functools

import jax
import jax.numpy as jnp
from jax import lax
from jax.experimental import pallas as pl
from jax.experimental.pallas import tpu as pltpu
from jax.sharding import PartitionSpec as P

CAP = 16
BASE = 256
LANES = 128
EXTRA = 8

logit_scale = 64.0
epsilon = 1e-06

VMEM = pl.BlockSpec(memory_space=pltpu.VMEM)


def split3(values):
    first = values.astype(jnp.bfloat16)
    rest = values - first.astype(jnp.float32)
    second = rest.astype(jnp.bfloat16)
    third = (rest - second.astype(jnp.float32)).astype(jnp.bfloat16)
    return first, second, third


def contract_lanes(left, right):
    return lax.dot_general(left, right, (((1,), (1,)), ((), ())), preferred_element_type=jnp.float32)


def slot_kernel(groups, slots, held, ids_ref, text_ref, out_ref, mark_ref, rank_ref):
    ids = ids_ref[...]
    pairs = ids.shape[1]
    group = lax.broadcasted_iota(jnp.int32, (groups, pairs), 0)
    start = group * held
    marks = jnp.where((ids >= start) & (ids < start + held), 1.0, 0.0)
    before = lax.broadcasted_iota(jnp.int32, (pairs, pairs), 0) < lax.broadcasted_iota(jnp.int32, (pairs, pairs), 1)
    triangle = jnp.where(before, 1.0, 0.0).astype(jnp.bfloat16)
    seen = jnp.dot(marks.astype(jnp.bfloat16), triangle, preferred_element_type=jnp.float32)
    rank = jnp.sum(marks * seen, axis=0, keepdims=True)
    owner = jnp.sum(marks * group.astype(jnp.float32), axis=0, keepdims=True)
    local = ids.astype(jnp.float32) - owner * held
    high = jnp.floor(local * (1.0 / BASE))
    low = local - high * BASE
    target = (owner * slots + rank).astype(jnp.int32)
    places = lax.broadcasted_iota(jnp.int32, (groups * slots, pairs), 0)
    chosen = jnp.where(places == target, 1.0, 0.0).astype(jnp.bfloat16)
    row = lax.broadcasted_iota(jnp.int32, (EXTRA, pairs), 0)
    digits = jnp.where(row == 0, low, jnp.where(row == 1, high + 1.0, 0.0)).astype(jnp.bfloat16)
    features = text_ref[...].T
    moved = contract_lanes(features, chosen).astype(jnp.bfloat16)
    named = contract_lanes(digits, chosen).astype(jnp.bfloat16)
    depth = features.shape[0]
    if slots % LANES == 0:
        for g in range(groups):
            out_ref[g, :depth, :] = moved[:, g * slots : (g + 1) * slots]
            out_ref[g, depth:, :] = named[:, g * slots : (g + 1) * slots]
    else:
        out_ref[:depth, :] = moved
        out_ref[depth:, :] = named
    mark_ref[...] = marks
    rank_ref[...] = rank


def read(ref, rows, at, width):
    if len(ref.shape) == 2:
        return ref[rows, at : at + width]
    slots = ref.shape[2]
    pieces = []
    while width:
        g, offset = divmod(at, slots)
        step = min(width, slots - offset)
        pieces.append(ref[g, rows, offset : offset + step])
        at, width = at + step, width - step
    return pieces[0] if len(pieces) == 1 else jnp.concatenate(pieces, axis=1)


def match_kernel(total, depth, arrived_ref, table_ref, part_ref, digit_ref):
    blocks = table_ref.shape[0]
    width = 2 * LANES if total % (2 * LANES) == 0 else LANES
    half = depth // 2 if depth % 32 == 0 else depth
    low_of = lax.broadcasted_iota(jnp.int32, (BASE, width), 0).astype(jnp.float32)
    for at in range(0, total, width):
        digits = read(arrived_ref, slice(depth, depth + EXTRA), at, width).astype(jnp.float32)
        low, high = digits[0:1], digits[1:2]
        lows = jnp.where(low_of == low, 1.0, 0.0).astype(jnp.bfloat16)
        dot = tsq = csq = jnp.zeros((1, width), jnp.float32)
        for top in range(0, depth, half):
            pieces = jnp.zeros((half, width), jnp.float32)
            for block in range(blocks):
                found = jnp.dot(table_ref[block, top : top + half, :], lows, preferred_element_type=jnp.float32)
                pieces = jnp.where(high == block + 1.0, found, pieces)
            floats = read(arrived_ref, slice(top, top + half), at, width).astype(jnp.float32)
            dot += jnp.sum(floats * pieces, axis=0, keepdims=True)
            tsq += jnp.sum(floats * floats, axis=0, keepdims=True)
            csq += jnp.sum(pieces * pieces, axis=0, keepdims=True)
        for step in range(width // LANES):
            lane = slice(step * LANES, (step + 1) * LANES)
            b = at // LANES + step
            for q, sums in enumerate((dot, tsq, csq)):
                part_ref[q, b : b + 1, :] = sums[:, lane]
            digit_ref[0, b : b + 1, :] = low[:, lane]
            digit_ref[1, b : b + 1, :] = high[:, lane]


def count_kernel(highs, *refs):
    *part_refs, digit_ref, out_ref = refs
    sums = [ref[...] for ref in part_refs]
    while len(sums) > 1:
        sums = [sums[i] + sums[i + 1] for i in range(0, len(sums), 2)]
    dot, tsq, csq = sums[0][0], sums[0][1], sums[0][2]
    match = jax.nn.sigmoid(logit_scale * dot * lax.rsqrt(tsq + epsilon) * lax.rsqrt(csq + epsilon))
    capped = CAP * 1.0
    blocks = match.shape[0]
    line = lambda rows: jnp.concatenate([rows[b : b + 1] for b in range(blocks)], axis=1)
    weights, low, high = line(match), line(digit_ref[0]), line(digit_ref[1])
    total = weights.shape[1]
    lows = jnp.where(lax.broadcasted_iota(jnp.int32, (BASE, total), 0).astype(jnp.float32) == low, 1.0, 0.0).astype(jnp.bfloat16)
    tops = jnp.where(lax.broadcasted_iota(jnp.int32, (highs, total), 0).astype(jnp.float32) + 1.0 == high, 1.0, 0.0)
    spread = jnp.concatenate(split3(tops * weights), axis=0)
    parts = contract_lanes(spread, lows)
    count = parts[:highs] + parts[highs : 2 * highs] + parts[2 * highs :]
    parts = jnp.dot(jnp.concatenate(split3(count), axis=0), lows, preferred_element_type=jnp.float32)
    looked = jnp.sum(tops * (parts[:highs] + parts[highs : 2 * highs] + parts[2 * highs :]), axis=0, keepdims=True)
    balanced = weights * capped / jnp.maximum(looked, capped)
    for b in range(blocks):
        out_ref[b : b + 1, :] = balanced[:, b * LANES : (b + 1) * LANES]


def unslot_kernel(returned_ref, mark_ref, rank_ref, out_ref):
    groups, slots = returned_ref.shape
    pairs = mark_ref.shape[1]
    ranks = lax.broadcasted_iota(jnp.int32, (slots, pairs), 0).astype(jnp.float32)
    chosen = jnp.where(ranks == rank_ref[...], 1.0, 0.0).astype(jnp.bfloat16)
    first, second, third = (jnp.dot(part, chosen, preferred_element_type=jnp.float32) for part in split3(returned_ref[...]))
    out_ref[...] = jnp.sum(mark_ref[...] * (first + second + third), axis=0, keepdims=True)


def body(text, concept_table, ids):
    groups = lax.axis_size("dp")
    quarters = lax.axis_size("concept")
    pairs, depth = text.shape
    held = concept_table.shape[0]
    slots = 2 * pairs // groups
    total = groups * slots
    f32 = jnp.float32
    blocks = -(-held // BASE)
    wide = slots % LANES == 0
    sent_shape = (groups, depth + EXTRA, slots) if wide else (depth + EXTRA, total)

    sent, marks, rank = pl.pallas_call(
        functools.partial(slot_kernel, groups, slots, held),
        out_shape=(
            jax.ShapeDtypeStruct(sent_shape, jnp.bfloat16),
            jax.ShapeDtypeStruct((groups, pairs), f32),
            jax.ShapeDtypeStruct((1, pairs), f32),
        ),
        in_specs=[VMEM] * 2,
        out_specs=(VMEM,) * 3,
        name="slot",
    )(ids.reshape(1, pairs), text)
    if not wide:
        sent = sent.reshape(depth + EXTRA, groups, slots).transpose(1, 0, 2)
    arrived = lax.all_to_all(sent, "dp", split_axis=0, concat_axis=0, tiled=True)
    if not wide:
        arrived = arrived.transpose(1, 0, 2).reshape(depth + EXTRA, total)

    padded = jnp.pad(concept_table, ((0, blocks * BASE - held), (0, 0)))
    turned = padded.reshape(blocks, BASE, depth).transpose(0, 2, 1)

    part, digits = pl.pallas_call(
        functools.partial(match_kernel, total, depth),
        out_shape=(
            jax.ShapeDtypeStruct((3, total // LANES, LANES), f32),
            jax.ShapeDtypeStruct((2, total // LANES, LANES), f32),
        ),
        in_specs=[VMEM] * 2,
        out_specs=(VMEM,) * 2,
        name="match",
    )(arrived, turned)

    if quarters & (quarters - 1) == 0:
        parts = [part] + [
            lax.ppermute(part, "concept", [(i, i ^ step) for i in range(quarters)]) for step in range(1, quarters)
        ]
    else:
        parts = [lax.psum(part, "concept")]

    balanced = pl.pallas_call(
        functools.partial(count_kernel, -(-blocks // 16) * 16),
        out_shape=jax.ShapeDtypeStruct((total // LANES, LANES), f32),
        in_specs=[VMEM] * (len(parts) + 1),
        out_specs=VMEM,
        name="count",
    )(*parts, digits)

    returned = lax.all_to_all(balanced.reshape(groups, slots), "dp", split_axis=0, concat_axis=0, tiled=True)

    out = pl.pallas_call(
        unslot_kernel,
        out_shape=jax.ShapeDtypeStruct((1, pairs), f32),
        in_specs=[VMEM] * 3,
        out_specs=VMEM,
        name="unslot",
    )(returned, marks, rank)
    return out.reshape(pairs)


def solution(mesh):
    placed = (P("dp", "concept"), P("dp", "concept"), P("dp"))
    return jax.shard_map(body, mesh=mesh, in_specs=placed, out_specs=P("dp"), check_vma=False)
```

```python
import functools

import jax
import jax.numpy as jnp
from jax import lax
from jax.experimental import pallas as pl
from jax.experimental.pallas import tpu as pltpu
from jax.sharding import PartitionSpec as P

CAP = 16
BASE = 256
LANES = 128
EXTRA = 8

logit_scale = 64.0
epsilon = 1e-06

VMEM = pl.BlockSpec(memory_space=pltpu.VMEM)
GRANT = pltpu.CompilerParams(vmem_limit_bytes=16 * 1024 * 1024)


def split3(values):
    first = values.astype(jnp.bfloat16)
    rest = values - first.astype(jnp.float32)
    second = rest.astype(jnp.bfloat16)
    third = (rest - second.astype(jnp.float32)).astype(jnp.bfloat16)
    return first, second, third


def contract_lanes(left, right):
    return lax.dot_general(left, right, (((1,), (1,)), ((), ())), preferred_element_type=jnp.float32)


def slot_kernel(groups, slots, held, ids_ref, text_ref, out_ref, mark_ref, rank_ref):
    ids = ids_ref[...]
    pairs = ids.shape[1]
    group = lax.broadcasted_iota(jnp.int32, (groups, pairs), 0)
    start = group * held
    marks = jnp.where((ids >= start) & (ids < start + held), 1.0, 0.0)
    before = lax.broadcasted_iota(jnp.int32, (pairs, pairs), 0) < lax.broadcasted_iota(jnp.int32, (pairs, pairs), 1)
    triangle = jnp.where(before, 1.0, 0.0).astype(jnp.bfloat16)
    seen = jnp.dot(marks.astype(jnp.bfloat16), triangle, preferred_element_type=jnp.float32)
    rank = jnp.sum(marks * seen, axis=0, keepdims=True)
    owner = jnp.sum(marks * group.astype(jnp.float32), axis=0, keepdims=True)
    local = ids.astype(jnp.float32) - owner * held
    high = jnp.floor(local * (1.0 / BASE))
    low = local - high * BASE
    target = (owner * slots + rank).astype(jnp.int32)
    places = lax.broadcasted_iota(jnp.int32, (groups * slots, pairs), 0)
    chosen = jnp.where(places == target, 1.0, 0.0).astype(jnp.bfloat16)
    row = lax.broadcasted_iota(jnp.int32, (EXTRA, pairs), 0)
    digits = jnp.where(row == 0, low, jnp.where(row == 1, high + 1.0, 0.0)).astype(jnp.bfloat16)
    features = text_ref[...].T
    moved = contract_lanes(features, chosen).astype(jnp.bfloat16)
    named = contract_lanes(digits, chosen).astype(jnp.bfloat16)
    depth = features.shape[0]
    if slots % LANES == 0:
        for g in range(groups):
            out_ref[g, :depth, :] = moved[:, g * slots : (g + 1) * slots]
            out_ref[g, depth:, :] = named[:, g * slots : (g + 1) * slots]
    else:
        out_ref[:depth, :] = moved
        out_ref[depth:, :] = named
    mark_ref[...] = marks
    rank_ref[...] = rank


def read(ref, rows, at, width):
    if len(ref.shape) == 2:
        return ref[rows, at : at + width]
    slots = ref.shape[2]
    pieces = []
    while width:
        g, offset = divmod(at, slots)
        step = min(width, slots - offset)
        pieces.append(ref[g, rows, offset : offset + step])
        at, width = at + step, width - step
    return pieces[0] if len(pieces) == 1 else jnp.concatenate(pieces, axis=1)


def match_kernel(total, depth, arrived_ref, table_ref, part_ref, digit_ref):
    blocks = table_ref.shape[0]
    width = 2 * LANES if total % (2 * LANES) == 0 else LANES
    half = depth // 2 if depth % 32 == 0 else depth
    low_of = lax.broadcasted_iota(jnp.int32, (BASE, width), 0).astype(jnp.float32)
    for at in range(0, total, width):
        digits = read(arrived_ref, slice(depth, depth + EXTRA), at, width).astype(jnp.float32)
        low, high = digits[0:1], digits[1:2]
        lows = jnp.where(low_of == low, 1.0, 0.0).astype(jnp.bfloat16)
        dot = tsq = csq = jnp.zeros((1, width), jnp.float32)
        for top in range(0, depth, half):
            pieces = jnp.zeros((half, width), jnp.float32)
            for block in range(blocks):
                found = jnp.dot(table_ref[block, top : top + half, :], lows, preferred_element_type=jnp.float32)
                pieces = jnp.where(high == block + 1.0, found, pieces)
            floats = read(arrived_ref, slice(top, top + half), at, width).astype(jnp.float32)
            dot += jnp.sum(floats * pieces, axis=0, keepdims=True)
            tsq += jnp.sum(floats * floats, axis=0, keepdims=True)
            csq += jnp.sum(pieces * pieces, axis=0, keepdims=True)
        for step in range(width // LANES):
            lane = slice(step * LANES, (step + 1) * LANES)
            b = at // LANES + step
            for q, sums in enumerate((dot, tsq, csq)):
                part_ref[q, b : b + 1, :] = sums[:, lane]
            digit_ref[0, b : b + 1, :] = low[:, lane]
            digit_ref[1, b : b + 1, :] = high[:, lane]


def count_kernel(highs, *refs):
    *part_refs, digit_ref, out_ref = refs
    sums = [ref[...] for ref in part_refs]
    while len(sums) > 1:
        sums = [sums[i] + sums[i + 1] for i in range(0, len(sums), 2)]
    dot, tsq, csq = sums[0][0], sums[0][1], sums[0][2]
    match = jax.nn.sigmoid(logit_scale * dot * lax.rsqrt(tsq + epsilon) * lax.rsqrt(csq + epsilon))
    capped = CAP * 1.0
    blocks = match.shape[0]
    line = lambda rows: jnp.concatenate([rows[b : b + 1] for b in range(blocks)], axis=1)
    weights, low, high = line(match), line(digit_ref[0]), line(digit_ref[1])
    total = weights.shape[1]
    lows = jnp.where(lax.broadcasted_iota(jnp.int32, (BASE, total), 0).astype(jnp.float32) == low, 1.0, 0.0).astype(jnp.bfloat16)
    tops = jnp.where(lax.broadcasted_iota(jnp.int32, (highs, total), 0).astype(jnp.float32) + 1.0 == high, 1.0, 0.0)
    spread = jnp.concatenate(split3(tops * weights), axis=0)
    parts = contract_lanes(spread, lows)
    count = parts[:highs] + parts[highs : 2 * highs] + parts[2 * highs :]
    parts = jnp.dot(jnp.concatenate(split3(count), axis=0), lows, preferred_element_type=jnp.float32)
    looked = jnp.sum(tops * (parts[:highs] + parts[highs : 2 * highs] + parts[2 * highs :]), axis=0, keepdims=True)
    balanced = weights * capped / jnp.maximum(looked, capped)
    for b in range(blocks):
        out_ref[b : b + 1, :] = balanced[:, b * LANES : (b + 1) * LANES]


def unslot_kernel(returned_ref, mark_ref, rank_ref, out_ref):
    groups, slots = returned_ref.shape
    pairs = mark_ref.shape[1]
    ranks = lax.broadcasted_iota(jnp.int32, (slots, pairs), 0).astype(jnp.float32)
    chosen = jnp.where(ranks == rank_ref[...], 1.0, 0.0).astype(jnp.bfloat16)
    first, second, third = (jnp.dot(part, chosen, preferred_element_type=jnp.float32) for part in split3(returned_ref[...]))
    out_ref[...] = jnp.sum(mark_ref[...] * (first + second + third), axis=0, keepdims=True)


def body(text, concept_table, ids):
    groups = lax.axis_size("dp")
    quarters = lax.axis_size("concept")
    pairs, depth = text.shape
    held = concept_table.shape[0]
    slots = 2 * pairs // groups
    total = groups * slots
    f32 = jnp.float32
    blocks = -(-held // BASE)
    wide = slots % LANES == 0
    sent_shape = (groups, depth + EXTRA, slots) if wide else (depth + EXTRA, total)

    sent, marks, rank = pl.pallas_call(
        functools.partial(slot_kernel, groups, slots, held),
        out_shape=(
            jax.ShapeDtypeStruct(sent_shape, jnp.bfloat16),
            jax.ShapeDtypeStruct((groups, pairs), f32),
            jax.ShapeDtypeStruct((1, pairs), f32),
        ),
        in_specs=[VMEM] * 2,
        out_specs=(VMEM,) * 3,
        name="slot",
    )(ids.reshape(1, pairs), text)
    if not wide:
        sent = sent.reshape(depth + EXTRA, groups, slots).transpose(1, 0, 2)
    arrived = lax.all_to_all(sent, "dp", split_axis=0, concat_axis=0, tiled=True)
    if not wide:
        arrived = arrived.transpose(1, 0, 2).reshape(depth + EXTRA, total)

    padded = jnp.pad(concept_table, ((0, blocks * BASE - held), (0, 0)))
    turned = padded.reshape(blocks, BASE, depth).transpose(0, 2, 1)

    part, digits = pl.pallas_call(
        functools.partial(match_kernel, total, depth),
        out_shape=(
            jax.ShapeDtypeStruct((3, total // LANES, LANES), f32),
            jax.ShapeDtypeStruct((2, total // LANES, LANES), f32),
        ),
        in_specs=[VMEM] * 2,
        out_specs=(VMEM,) * 2,
        compiler_params=GRANT,
        name="match",
    )(arrived, turned)

    if quarters & (quarters - 1) == 0:
        parts = [part] + [
            lax.ppermute(part, "concept", [(i, i ^ step) for i in range(quarters)]) for step in range(1, quarters)
        ]
    else:
        parts = [lax.psum(part, "concept")]

    balanced = pl.pallas_call(
        functools.partial(count_kernel, -(-blocks // 16) * 16),
        out_shape=jax.ShapeDtypeStruct((total // LANES, LANES), f32),
        in_specs=[VMEM] * (len(parts) + 1),
        out_specs=VMEM,
        compiler_params=GRANT,
        name="count",
    )(*parts, digits)

    returned = lax.all_to_all(balanced.reshape(groups, slots), "dp", split_axis=0, concat_axis=0, tiled=True)

    out = pl.pallas_call(
        unslot_kernel,
        out_shape=jax.ShapeDtypeStruct((1, pairs), f32),
        in_specs=[VMEM] * 3,
        out_specs=VMEM,
        compiler_params=GRANT,
        name="unslot",
    )(returned, marks, rank)
    return out.reshape(pairs)


def solution(mesh):
    placed = (P("dp", "concept"), P("dp", "concept"), P("dp"))
    return jax.shard_map(body, mesh=mesh, in_specs=placed, out_specs=P("dp"), check_vma=False)
```

```python
import functools

import jax
import jax.numpy as jnp
from jax import lax
from jax.experimental import pallas as pl
from jax.experimental.pallas import tpu as pltpu
from jax.sharding import PartitionSpec as P


CAP = 16
BASE = 256
LANES = 128
EXTRA = 8
FEW = (2, 4, 8)
ORDER = (6, 4, 2, 7, 5, 3, 1)


logit_scale = 64.0
epsilon = 1e-06

VMEM = pl.BlockSpec(memory_space=pltpu.VMEM)
GRANT = pltpu.CompilerParams(vmem_limit_bytes=16 * 1024 * 1024)


def split3(values):
    first = values.astype(jnp.bfloat16)
    rest = values - first.astype(jnp.float32)
    second = rest.astype(jnp.bfloat16)
    third = (rest - second.astype(jnp.float32)).astype(jnp.bfloat16)
    return first, second, third


def contract_lanes(left, right):
    return lax.dot_general(left, right, (((1,), (1,)), ((), ())), preferred_element_type=jnp.float32)


def rank_kernel(groups, held, wide, ids_ref, digit_ref, partner_ref, mark_ref, rank_ref):
    ids = ids_ref[...].astype(jnp.int32)
    pairs = ids.shape[1]
    me = lax.axis_index("dp") if wide else 0
    before = lax.broadcasted_iota(jnp.int32, (pairs, pairs), 0) < lax.broadcasted_iota(jnp.int32, (pairs, pairs), 1)
    triangle = jnp.where(before, 1.0, 0.0).astype(jnp.bfloat16)
    group = lax.broadcasted_iota(jnp.int32, (groups, pairs), 0)
    start = group * held
    marks = jnp.where((ids >= start) & (ids < start + held), 1.0, 0.0)
    partner = (group ^ me) * held
    partner_ref[...] = jnp.where((ids >= partner) & (ids < partner + held), 1.0, 0.0)
    seen = jnp.dot(marks.astype(jnp.bfloat16), triangle, preferred_element_type=jnp.float32)
    local = ids.astype(jnp.float32) - jnp.sum(marks * start.astype(jnp.float32), axis=0, keepdims=True)
    high = jnp.floor(local * (1.0 / BASE))
    row = lax.broadcasted_iota(jnp.int32, (EXTRA, pairs), 0)
    digit_ref[...] = jnp.where(row == 0, local - high * BASE, jnp.where(row == 1, high + 1.0, 0.0))
    mark_ref[...] = marks
    rank_ref[...] = jnp.sum(marks * seen, axis=0, keepdims=True)


def slot_kernel(groups, slots, wide, text_ref, digit_ref, partner_ref, rank_ref, *out_refs):
    pairs = text_ref.shape[0]
    marks, rank = partner_ref[...], rank_ref[...]
    if wide:
        ranks = lax.broadcasted_iota(jnp.int32, (slots, pairs), 0).astype(jnp.float32)
        ranked = jnp.where(ranks == rank, 1.0, 0.0).astype(jnp.bfloat16)
        marked = marks.astype(jnp.bfloat16)
        chosen = jnp.concatenate([ranked * marked[g : g + 1] for g in range(groups)], axis=0)
    else:
        group = lax.broadcasted_iota(jnp.int32, (groups, pairs), 0)
        target = jnp.sum(marks * (group * slots).astype(jnp.float32), axis=0, keepdims=True) + rank
        places = lax.broadcasted_iota(jnp.int32, (groups * slots, pairs), 0).astype(jnp.float32)
        chosen = jnp.where(places == target, 1.0, 0.0).astype(jnp.bfloat16)
    features = jnp.concatenate([text_ref[...].T, digit_ref[...].astype(jnp.bfloat16)], axis=0)
    moved = contract_lanes(features, chosen).astype(jnp.bfloat16)
    width = out_refs[0].shape[1]
    for g, out_ref in enumerate(out_refs):
        out_ref[...] = moved[:, g * width : (g + 1) * width]


def turn_kernel(table_ref, out_ref):
    for block in range(out_ref.shape[0]):
        out_ref[block] = table_ref[block * BASE : (block + 1) * BASE, :].T


def match_kernel(arrivals, depth, *refs):
    *in_refs, part_ref, digit_ref = refs
    arrived_refs, table_ref, earlier_refs = in_refs[:arrivals], in_refs[arrivals], in_refs[arrivals + 1 :]
    done = 0
    for i in range(0, len(earlier_refs), 2):
        count = earlier_refs[i].shape[1]
        part_ref[:, done : done + count, :] = earlier_refs[i][...]
        digit_ref[:, done : done + count, :] = earlier_refs[i + 1][...]
        done += count
    blocks = table_ref.shape[0]
    chunks = [(ref, at) for ref in arrived_refs for at in range(0, ref.shape[1], LANES)]
    pack = 2 if len(chunks) % 2 == 0 else 1
    width = pack * LANES
    half = depth // 2 if depth % 32 == 0 else depth
    low_of = lax.broadcasted_iota(jnp.int32, (BASE, width), 0).astype(jnp.float32)
    for first in range(0, len(chunks), pack):

        def read(rows):
            pieces = [ref[rows, at : at + LANES] for ref, at in chunks[first : first + pack]]
            return pieces[0] if pack == 1 else jnp.concatenate(pieces, axis=1)

        digits = read(slice(depth, depth + EXTRA)).astype(jnp.float32)
        low, high = digits[0:1], digits[1:2]
        lows = jnp.where(low_of == low, 1.0, 0.0).astype(jnp.bfloat16)
        dot = tsq = csq = jnp.zeros((1, width), jnp.float32)
        for top in range(0, depth, half):
            pieces = jnp.zeros((half, width), jnp.float32)
            for block in range(blocks):
                found = jnp.dot(table_ref[block, top : top + half, :], lows, preferred_element_type=jnp.float32)
                pieces = jnp.where(high == block + 1.0, found, pieces)
            floats = read(slice(top, top + half)).astype(jnp.float32)
            dot += jnp.sum(floats * pieces, axis=0, keepdims=True)
            tsq += jnp.sum(floats * floats, axis=0, keepdims=True)
            csq += jnp.sum(pieces * pieces, axis=0, keepdims=True)
        for step in range(pack):
            lane = slice(step * LANES, (step + 1) * LANES)
            b = done + first + step
            for q, sums in enumerate((dot, tsq, csq)):
                part_ref[q, b : b + 1, :] = sums[:, lane]
            digit_ref[0, b : b + 1, :] = low[:, lane]
            digit_ref[1, b : b + 1, :] = high[:, lane]


def match(arrived, table, depth, earlier):
    count = sum(array.shape[1] for array in arrived) // LANES
    count += sum(pair[0].shape[1] for pair in earlier)
    operands = (*arrived, table, *(array for pair in earlier for array in pair))
    return pl.pallas_call(
        functools.partial(match_kernel, len(arrived), depth),
        out_shape=(
            jax.ShapeDtypeStruct((3, count, LANES), jnp.float32),
            jax.ShapeDtypeStruct((2, count, LANES), jnp.float32),
        ),
        in_specs=[VMEM] * len(operands),
        out_specs=(VMEM,) * 2,
        compiler_params=GRANT,
        name="match",
    )(*operands)


def line(rows):
    return jnp.concatenate([rows[b : b + 1] for b in range(rows.shape[0])], axis=1)


def prepare_kernel(digit_ref, rank_ref, low_ref, turned_ref, top_ref, chosen_ref):
    low, high = line(digit_ref[0]), line(digit_ref[1])
    lows = lax.broadcasted_iota(jnp.int32, low_ref.shape, 0).astype(jnp.float32) == low
    low_ref[...] = jnp.where(lows, 1.0, 0.0).astype(jnp.bfloat16)
    turned_ref[...] = low_ref[...].T
    tops = lax.broadcasted_iota(jnp.int32, top_ref.shape, 0).astype(jnp.float32) + 1.0 == high
    top_ref[...] = jnp.where(tops, 1.0, 0.0)
    ranks = lax.broadcasted_iota(jnp.int32, chosen_ref.shape, 0).astype(jnp.float32)
    chosen_ref[...] = jnp.where(ranks == rank_ref[...], 1.0, 0.0).astype(jnp.bfloat16)


def join3(parts):
    rows = parts.shape[0] // 3
    return parts[:rows] + parts[rows : 2 * rows] + parts[2 * rows :]


def count_kernel(places, *refs):
    *part_refs, low_ref, turned_ref, top_ref, out_ref = refs
    sums = [ref[...] for ref in part_refs]
    while len(sums) > 1:
        sums = [sums[i] + sums[i + 1] for i in range(0, len(sums), 2)]
    dot, tsq, csq = sums[0][0], sums[0][1], sums[0][2]
    match = jax.nn.sigmoid(logit_scale * dot * lax.rsqrt(tsq + epsilon) * lax.rsqrt(csq + epsilon))
    capped = CAP * 1.0
    weights, tops = line(match), top_ref[...]
    spread = jnp.concatenate(split3(tops * weights), axis=0)
    count = join3(jnp.dot(spread, turned_ref[...], preferred_element_type=jnp.float32))
    parts = jnp.dot(jnp.concatenate(split3(count), axis=0), low_ref[...], preferred_element_type=jnp.float32)
    looked = jnp.sum(tops * join3(parts), axis=0, keepdims=True)
    balanced = weights * capped / jnp.maximum(looked, capped)
    blocks = match.shape[0]
    each = blocks // len(places) if places else 0
    for b in range(blocks):
        to = (lax.axis_index("dp") ^ places[b // each]) * each + b % each if places else b
        out_ref[pl.ds(to, 1), :] = balanced[:, b * LANES : (b + 1) * LANES]


def unslot_kernel(returned_ref, mark_ref, chosen_ref, out_ref):
    spread = jnp.concatenate(split3(returned_ref[...]), axis=0)
    found = join3(jnp.dot(spread, chosen_ref[...], preferred_element_type=jnp.float32))
    out_ref[...] = jnp.sum(mark_ref[...] * found, axis=0, keepdims=True)


def hops(groups):
    return tuple(step for step in ORDER if step < groups)


def chunks(groups):
    *far, near = hops(groups)
    middle = len(far) // 2
    line = (0, *far[:middle], near, *far[middle:])
    return tuple(zip(line[::2], line[1::2]))


def body(text, concept_table, ids):
    groups = lax.axis_size("dp")
    quarters = lax.axis_size("concept")
    pairs, depth = text.shape
    held = concept_table.shape[0]
    slots = 2 * pairs // groups
    total = groups * slots
    f32 = jnp.float32
    blocks = -(-held // BASE)
    wide = slots % LANES == 0 and groups in FEW

    padded = jnp.pad(concept_table, ((0, blocks * BASE - held), (0, 0)))
    turned = pl.pallas_call(
        turn_kernel,
        out_shape=jax.ShapeDtypeStruct((blocks, depth, BASE), jnp.bfloat16),
        in_specs=[VMEM],
        out_specs=VMEM,
        compiler_params=GRANT,
        name="turn",
    )(padded)

    columns = slots if wide else total
    sheets = groups if wide else 1
    digits, partners, marks, rank = pl.pallas_call(
        functools.partial(rank_kernel, groups, held, wide),
        out_shape=(
            jax.ShapeDtypeStruct((EXTRA, pairs), f32),
            jax.ShapeDtypeStruct((groups, pairs), f32),
            jax.ShapeDtypeStruct((groups, pairs), f32),
            jax.ShapeDtypeStruct((1, pairs), f32),
        ),
        in_specs=[VMEM],
        out_specs=(VMEM,) * 4,
        compiler_params=GRANT,
        cost_estimate=pl.CostEstimate(flops=5 * 10**8, bytes_accessed=4 * pairs * groups, transcendentals=0),
        name="rank",
    )(ids.astype(f32).reshape(1, pairs))
    sent = pl.pallas_call(
        functools.partial(slot_kernel, groups, slots, wide),
        out_shape=[jax.ShapeDtypeStruct((depth + EXTRA, columns), jnp.bfloat16)] * sheets,
        in_specs=[VMEM] * 4,
        out_specs=[VMEM] * sheets,
        compiler_params=GRANT,
        name="slot",
    )(text, digits, partners, rank)
    if wide:
        arrived = {0: sent[0]}
        for step in hops(groups):
            arrived[step] = lax.ppermute(sent[step], "dp", [(i, i ^ step) for i in range(groups)])
        part = digits = None
        for chunk in chunks(groups):
            earlier = [] if part is None else [(part, digits)]
            part, digits = match([arrived[step] for step in chunk], turned, depth, earlier)
        places = tuple(step for chunk in chunks(groups) for step in chunk)
    else:
        split = sent[0].reshape(depth + EXTRA, groups, slots).transpose(1, 0, 2)
        joined = lax.all_to_all(split, "dp", split_axis=0, concat_axis=0, tiled=True)
        joined = joined.transpose(1, 0, 2).reshape(depth + EXTRA, total)
        part, digits = match([joined], turned, depth, [])
        places = None

    if quarters & (quarters - 1) == 0:
        parts = [part]
        for step in range(1, quarters):
            parts.append(lax.ppermute(part, "concept", [(i, i ^ step) for i in range(quarters)]))
    else:
        parts = [lax.psum(part, "concept")]

    highs = -(-blocks // 16) * 16
    tables = pl.pallas_call(
        prepare_kernel,
        out_shape=(
            jax.ShapeDtypeStruct((BASE, total), jnp.bfloat16),
            jax.ShapeDtypeStruct((total, BASE), jnp.bfloat16),
            jax.ShapeDtypeStruct((highs, total), f32),
            jax.ShapeDtypeStruct((slots, pairs), jnp.bfloat16),
        ),
        in_specs=[VMEM] * 2,
        out_specs=(VMEM,) * 4,
        compiler_params=GRANT,
        name="prepare",
    )(digits, rank)
    *tables, chosen = tables
    balanced = pl.pallas_call(
        functools.partial(count_kernel, places),
        out_shape=jax.ShapeDtypeStruct((total // LANES, LANES), f32),
        in_specs=[VMEM] * (len(parts) + 3),
        out_specs=VMEM,
        compiler_params=GRANT,
        name="count",
    )(*parts, *tables)

    returned = lax.all_to_all(balanced.reshape(groups, slots), "dp", split_axis=0, concat_axis=0, tiled=True)

    out = pl.pallas_call(
        unslot_kernel,
        out_shape=jax.ShapeDtypeStruct((1, pairs), f32),
        in_specs=[VMEM] * 3,
        out_specs=VMEM,
        compiler_params=GRANT,
        name="unslot",
    )(returned, marks, chosen)
    return out.reshape(pairs)


def solution(mesh):
    placed = (P("dp", "concept"), P("dp", "concept"), P("dp"))
    return jax.shard_map(body, mesh=mesh, in_specs=placed, out_specs=P("dp"), check_vma=False)
```

```python
import functools

import jax
import jax.numpy as jnp
from jax import lax
from jax.experimental import pallas as pl
from jax.experimental.pallas import tpu as pltpu
from jax.sharding import PartitionSpec as P


CAP = 16
BASE = 256
LANES = 128
EXTRA = 8
FEW = (2, 4, 8)
ORDER = (6, 7, 2, 1, 4, 3, 5)


logit_scale = 64.0
epsilon = 1e-06

VMEM = pl.BlockSpec(memory_space=pltpu.VMEM)
GRANT = pltpu.CompilerParams(vmem_limit_bytes=16 * 1024 * 1024)


def split3(values):
    first = values.astype(jnp.bfloat16)
    rest = values - first.astype(jnp.float32)
    second = rest.astype(jnp.bfloat16)
    third = (rest - second.astype(jnp.float32)).astype(jnp.bfloat16)
    return first, second, third


def contract_lanes(left, right):
    return lax.dot_general(left, right, (((1,), (1,)), ((), ())), preferred_element_type=jnp.float32)


def rank_kernel(groups, held, wide, ids_ref, digit_ref, partner_ref, mark_ref, rank_ref):
    ids = ids_ref[...].astype(jnp.int32)
    pairs = ids.shape[1]
    me = lax.axis_index("dp") if wide else 0
    before = lax.broadcasted_iota(jnp.int32, (pairs, pairs), 0) < lax.broadcasted_iota(jnp.int32, (pairs, pairs), 1)
    triangle = jnp.where(before, 1.0, 0.0).astype(jnp.bfloat16)
    group = lax.broadcasted_iota(jnp.int32, (groups, pairs), 0)
    start = group * held
    marks = jnp.where((ids >= start) & (ids < start + held), 1.0, 0.0)
    partner = (group ^ me) * held
    partner_ref[...] = jnp.where((ids >= partner) & (ids < partner + held), 1.0, 0.0)
    seen = jnp.dot(marks.astype(jnp.bfloat16), triangle, preferred_element_type=jnp.float32)
    local = ids.astype(jnp.float32) - jnp.sum(marks * start.astype(jnp.float32), axis=0, keepdims=True)
    high = jnp.floor(local * (1.0 / BASE))
    row = lax.broadcasted_iota(jnp.int32, (EXTRA, pairs), 0)
    digit_ref[...] = jnp.where(row == 0, local - high * BASE, jnp.where(row == 1, high + 1.0, 0.0))
    mark_ref[...] = marks
    rank_ref[...] = jnp.sum(marks * seen, axis=0, keepdims=True)


def slot_kernel(groups, slots, wide, text_ref, digit_ref, partner_ref, rank_ref, *out_refs):
    pairs = text_ref.shape[0]
    marks, rank = partner_ref[...], rank_ref[...]
    if wide:
        ranks = lax.broadcasted_iota(jnp.int32, (slots, pairs), 0).astype(jnp.float32)
        ranked = jnp.where(ranks == rank, 1.0, 0.0).astype(jnp.bfloat16)
        marked = marks.astype(jnp.bfloat16)
        chosen = jnp.concatenate([ranked * marked[g : g + 1] for g in range(groups)], axis=0)
    else:
        group = lax.broadcasted_iota(jnp.int32, (groups, pairs), 0)
        target = jnp.sum(marks * (group * slots).astype(jnp.float32), axis=0, keepdims=True) + rank
        places = lax.broadcasted_iota(jnp.int32, (groups * slots, pairs), 0).astype(jnp.float32)
        chosen = jnp.where(places == target, 1.0, 0.0).astype(jnp.bfloat16)
    features = jnp.concatenate([text_ref[...].T, digit_ref[...].astype(jnp.bfloat16)], axis=0)
    moved = contract_lanes(features, chosen).astype(jnp.bfloat16)
    width = out_refs[0].shape[1]
    for g, out_ref in enumerate(out_refs):
        out_ref[...] = moved[:, g * width : (g + 1) * width]


def turn_kernel(table_ref, out_ref):
    for block in range(out_ref.shape[0]):
        out_ref[block] = table_ref[block * BASE : (block + 1) * BASE, :].T


def match_kernel(arrivals, depth, *refs):
    *in_refs, part_ref, digit_ref = refs
    arrived_refs, table_ref, earlier_refs = in_refs[:arrivals], in_refs[arrivals], in_refs[arrivals + 1 :]
    done = 0
    for i in range(0, len(earlier_refs), 2):
        count = earlier_refs[i].shape[1]
        part_ref[:, done : done + count, :] = earlier_refs[i][...]
        digit_ref[:, done : done + count, :] = earlier_refs[i + 1][...]
        done += count
    blocks = table_ref.shape[0]
    chunks = [(ref, at) for ref in arrived_refs for at in range(0, ref.shape[1], LANES)]
    pack = 2 if len(chunks) % 2 == 0 else 1
    width = pack * LANES
    half = depth // 2 if depth % 32 == 0 else depth
    low_of = lax.broadcasted_iota(jnp.int32, (BASE, width), 0).astype(jnp.float32)
    for first in range(0, len(chunks), pack):

        def read(rows):
            pieces = [ref[rows, at : at + LANES] for ref, at in chunks[first : first + pack]]
            return pieces[0] if pack == 1 else jnp.concatenate(pieces, axis=1)

        digits = read(slice(depth, depth + EXTRA)).astype(jnp.float32)
        low, high = digits[0:1], digits[1:2]
        lows = jnp.where(low_of == low, 1.0, 0.0).astype(jnp.bfloat16)
        dot = tsq = csq = jnp.zeros((1, width), jnp.float32)
        for top in range(0, depth, half):
            pieces = jnp.zeros((half, width), jnp.float32)
            for block in range(blocks):
                found = jnp.dot(table_ref[block, top : top + half, :], lows, preferred_element_type=jnp.float32)
                pieces = jnp.where(high == block + 1.0, found, pieces)
            floats = read(slice(top, top + half)).astype(jnp.float32)
            dot += jnp.sum(floats * pieces, axis=0, keepdims=True)
            tsq += jnp.sum(floats * floats, axis=0, keepdims=True)
            csq += jnp.sum(pieces * pieces, axis=0, keepdims=True)
        for step in range(pack):
            lane = slice(step * LANES, (step + 1) * LANES)
            b = done + first + step
            for q, sums in enumerate((dot, tsq, csq)):
                part_ref[q, b : b + 1, :] = sums[:, lane]
            digit_ref[0, b : b + 1, :] = low[:, lane]
            digit_ref[1, b : b + 1, :] = high[:, lane]


def match(arrived, table, depth, earlier):
    count = sum(array.shape[1] for array in arrived) // LANES
    count += sum(pair[0].shape[1] for pair in earlier)
    operands = (*arrived, table, *(array for pair in earlier for array in pair))
    return pl.pallas_call(
        functools.partial(match_kernel, len(arrived), depth),
        out_shape=(
            jax.ShapeDtypeStruct((3, count, LANES), jnp.float32),
            jax.ShapeDtypeStruct((2, count, LANES), jnp.float32),
        ),
        in_specs=[VMEM] * len(operands),
        out_specs=(VMEM,) * 2,
        compiler_params=GRANT,
        name="match",
    )(*operands)


def line(rows):
    return jnp.concatenate([rows[b : b + 1] for b in range(rows.shape[0])], axis=1)


def prepare_kernel(digit_ref, rank_ref, low_ref, turned_ref, top_ref, chosen_ref):
    low, high = line(digit_ref[0]), line(digit_ref[1])
    lows = lax.broadcasted_iota(jnp.int32, low_ref.shape, 0).astype(jnp.float32) == low
    low_ref[...] = jnp.where(lows, 1.0, 0.0).astype(jnp.bfloat16)
    turned_ref[...] = low_ref[...].T
    tops = lax.broadcasted_iota(jnp.int32, top_ref.shape, 0).astype(jnp.float32) + 1.0 == high
    top_ref[...] = jnp.where(tops, 1.0, 0.0)
    ranks = lax.broadcasted_iota(jnp.int32, chosen_ref.shape, 0).astype(jnp.float32)
    chosen_ref[...] = jnp.where(ranks == rank_ref[...], 1.0, 0.0).astype(jnp.bfloat16)


def join3(parts):
    rows = parts.shape[0] // 3
    return parts[:rows] + parts[rows : 2 * rows] + parts[2 * rows :]


def count_kernel(places, *refs):
    *part_refs, low_ref, turned_ref, top_ref, out_ref = refs
    sums = [ref[...] for ref in part_refs]
    while len(sums) > 1:
        sums = [sums[i] + sums[i + 1] for i in range(0, len(sums), 2)]
    dot, tsq, csq = sums[0][0], sums[0][1], sums[0][2]
    match = jax.nn.sigmoid(logit_scale * dot * lax.rsqrt(tsq + epsilon) * lax.rsqrt(csq + epsilon))
    capped = CAP * 1.0
    weights, tops = line(match), top_ref[...]
    spread = jnp.concatenate(split3(tops * weights), axis=0)
    count = join3(jnp.dot(spread, turned_ref[...], preferred_element_type=jnp.float32))
    parts = jnp.dot(jnp.concatenate(split3(count), axis=0), low_ref[...], preferred_element_type=jnp.float32)
    looked = jnp.sum(tops * join3(parts), axis=0, keepdims=True)
    balanced = weights * capped / jnp.maximum(looked, capped)
    blocks = match.shape[0]
    each = blocks // len(places) if places else 0
    for b in range(blocks):
        to = (lax.axis_index("dp") ^ places[b // each]) * each + b % each if places else b
        out_ref[pl.ds(to, 1), :] = balanced[:, b * LANES : (b + 1) * LANES]


def unslot_kernel(returned_ref, mark_ref, chosen_ref, out_ref):
    spread = jnp.concatenate(split3(returned_ref[...]), axis=0)
    found = join3(jnp.dot(spread, chosen_ref[...], preferred_element_type=jnp.float32))
    out_ref[...] = jnp.sum(mark_ref[...] * found, axis=0, keepdims=True)


def hops(groups):
    return tuple(step for step in ORDER if step < groups)


def chunks(groups):
    line = (0, *hops(groups))
    return tuple(zip(line[::2], line[1::2]))


def body(text, concept_table, ids):
    groups = lax.axis_size("dp")
    quarters = lax.axis_size("concept")
    pairs, depth = text.shape
    held = concept_table.shape[0]
    slots = 2 * pairs // groups
    total = groups * slots
    f32 = jnp.float32
    blocks = -(-held // BASE)
    wide = slots % LANES == 0 and groups in FEW

    padded = jnp.pad(concept_table, ((0, blocks * BASE - held), (0, 0)))
    turned = pl.pallas_call(
        turn_kernel,
        out_shape=jax.ShapeDtypeStruct((blocks, depth, BASE), jnp.bfloat16),
        in_specs=[VMEM],
        out_specs=VMEM,
        compiler_params=GRANT,
        name="turn",
    )(padded)

    columns = slots if wide else total
    sheets = groups if wide else 1
    digits, partners, marks, rank = pl.pallas_call(
        functools.partial(rank_kernel, groups, held, wide),
        out_shape=(
            jax.ShapeDtypeStruct((EXTRA, pairs), f32),
            jax.ShapeDtypeStruct((groups, pairs), f32),
            jax.ShapeDtypeStruct((groups, pairs), f32),
            jax.ShapeDtypeStruct((1, pairs), f32),
        ),
        in_specs=[VMEM],
        out_specs=(VMEM,) * 4,
        compiler_params=GRANT,
        cost_estimate=pl.CostEstimate(flops=5 * 10**8, bytes_accessed=4 * pairs * groups, transcendentals=0),
        name="rank",
    )(ids.astype(f32).reshape(1, pairs))
    sent = pl.pallas_call(
        functools.partial(slot_kernel, groups, slots, wide),
        out_shape=[jax.ShapeDtypeStruct((depth + EXTRA, columns), jnp.bfloat16)] * sheets,
        in_specs=[VMEM] * 4,
        out_specs=[VMEM] * sheets,
        compiler_params=GRANT,
        name="slot",
    )(text, digits, partners, rank)
    if wide:
        arrived = {0: sent[0]}
        for step in hops(groups):
            arrived[step] = lax.ppermute(sent[step], "dp", [(i, i ^ step) for i in range(groups)])
        part = digits = None
        for chunk in chunks(groups):
            earlier = [] if part is None else [(part, digits)]
            part, digits = match([arrived[step] for step in chunk], turned, depth, earlier)
        places = tuple(step for chunk in chunks(groups) for step in chunk)
    else:
        split = sent[0].reshape(depth + EXTRA, groups, slots).transpose(1, 0, 2)
        joined = lax.all_to_all(split, "dp", split_axis=0, concat_axis=0, tiled=True)
        joined = joined.transpose(1, 0, 2).reshape(depth + EXTRA, total)
        part, digits = match([joined], turned, depth, [])
        places = None

    if quarters & (quarters - 1) == 0:
        parts = [part]
        for step in range(1, quarters):
            parts.append(lax.ppermute(part, "concept", [(i, i ^ step) for i in range(quarters)]))
    else:
        parts = [lax.psum(part, "concept")]

    highs = -(-blocks // 16) * 16
    tables = pl.pallas_call(
        prepare_kernel,
        out_shape=(
            jax.ShapeDtypeStruct((BASE, total), jnp.bfloat16),
            jax.ShapeDtypeStruct((total, BASE), jnp.bfloat16),
            jax.ShapeDtypeStruct((highs, total), f32),
            jax.ShapeDtypeStruct((slots, pairs), jnp.bfloat16),
        ),
        in_specs=[VMEM] * 2,
        out_specs=(VMEM,) * 4,
        compiler_params=GRANT,
        name="prepare",
    )(digits, rank)
    *tables, chosen = tables
    balanced = pl.pallas_call(
        functools.partial(count_kernel, places),
        out_shape=jax.ShapeDtypeStruct((total // LANES, LANES), f32),
        in_specs=[VMEM] * (len(parts) + 3),
        out_specs=VMEM,
        compiler_params=GRANT,
        name="count",
    )(*parts, *tables)

    returned = lax.all_to_all(balanced.reshape(groups, slots), "dp", split_axis=0, concat_axis=0, tiled=True)

    out = pl.pallas_call(
        unslot_kernel,
        out_shape=jax.ShapeDtypeStruct((1, pairs), f32),
        in_specs=[VMEM] * 3,
        out_specs=VMEM,
        compiler_params=GRANT,
        name="unslot",
    )(returned, marks, chosen)
    return out.reshape(pairs)


def solution(mesh):
    placed = (P("dp", "concept"), P("dp", "concept"), P("dp"))
    return jax.shard_map(body, mesh=mesh, in_specs=placed, out_specs=P("dp"), check_vma=False)
```

```python
import functools

import jax
import jax.numpy as jnp
from jax import lax
from jax.experimental import pallas as pl
from jax.experimental.pallas import tpu as pltpu
from jax.sharding import PartitionSpec as P


CAP = 16
BASE = 256
LANES = 128
EXTRA = 8
FEW = (2, 4, 8)
ORDER = (6, 7, 2, 1, 4, 3, 5)


logit_scale = 64.0
epsilon = 1e-06

VMEM = pl.BlockSpec(memory_space=pltpu.VMEM)
GRANT = pltpu.CompilerParams(vmem_limit_bytes=16 * 1024 * 1024)


def split3(values):
    first = values.astype(jnp.bfloat16)
    rest = values - first.astype(jnp.float32)
    second = rest.astype(jnp.bfloat16)
    third = (rest - second.astype(jnp.float32)).astype(jnp.bfloat16)
    return first, second, third


def contract_lanes(left, right):
    return lax.dot_general(left, right, (((1,), (1,)), ((), ())), preferred_element_type=jnp.float32)


def rank_kernel(groups, held, wide, ids_ref, digit_ref, partner_ref, mark_ref, rank_ref):
    ids = ids_ref[...]
    pairs = ids.shape[1]
    me = lax.axis_index("dp") if wide else 0
    before = lax.broadcasted_iota(jnp.int32, (pairs, pairs), 0) < lax.broadcasted_iota(jnp.int32, (pairs, pairs), 1)
    triangle = jnp.where(before, 1.0, 0.0).astype(jnp.bfloat16)
    group = lax.broadcasted_iota(jnp.int32, (groups, pairs), 0)
    start = group * held
    marks = jnp.where((ids >= start) & (ids < start + held), 1.0, 0.0)
    partner = (group ^ me) * held
    partner_ref[...] = jnp.where((ids >= partner) & (ids < partner + held), 1.0, 0.0)
    seen = jnp.dot(marks.astype(jnp.bfloat16), triangle, preferred_element_type=jnp.float32)
    local = ids.astype(jnp.float32) - jnp.sum(marks * start.astype(jnp.float32), axis=0, keepdims=True)
    high = jnp.floor(local * (1.0 / BASE))
    row = lax.broadcasted_iota(jnp.int32, (EXTRA, pairs), 0)
    digit_ref[...] = jnp.where(row == 0, local - high * BASE, jnp.where(row == 1, high + 1.0, 0.0))
    mark_ref[...] = marks
    rank_ref[...] = jnp.sum(marks * seen, axis=0, keepdims=True)


def slot_kernel(groups, slots, wide, text_ref, digit_ref, partner_ref, rank_ref, *out_refs):
    pairs = text_ref.shape[0]
    marks, rank = partner_ref[...], rank_ref[...]
    if wide:
        ranks = lax.broadcasted_iota(jnp.int32, (slots, pairs), 0).astype(jnp.float32)
        ranked = jnp.where(ranks == rank, 1.0, 0.0).astype(jnp.bfloat16)
        marked = marks.astype(jnp.bfloat16)
        chosen = jnp.concatenate([ranked * marked[g : g + 1] for g in range(groups)], axis=0)
    else:
        group = lax.broadcasted_iota(jnp.int32, (groups, pairs), 0)
        target = jnp.sum(marks * (group * slots).astype(jnp.float32), axis=0, keepdims=True) + rank
        places = lax.broadcasted_iota(jnp.int32, (groups * slots, pairs), 0).astype(jnp.float32)
        chosen = jnp.where(places == target, 1.0, 0.0).astype(jnp.bfloat16)
    features = jnp.concatenate([text_ref[...].T, digit_ref[...].astype(jnp.bfloat16)], axis=0)
    moved = contract_lanes(features, chosen).astype(jnp.bfloat16)
    width = out_refs[0].shape[1]
    for g, out_ref in enumerate(out_refs):
        out_ref[...] = moved[:, g * width : (g + 1) * width]


def match_kernel(arrivals, depth, turn, *refs):
    if turn:
        *refs, turned_ref = refs
    *in_refs, part_ref, digit_ref = refs
    arrived_refs, table_ref, earlier_refs = in_refs[:arrivals], in_refs[arrivals], in_refs[arrivals + 1 :]
    done = 0
    for i in range(0, len(earlier_refs), 2):
        count = earlier_refs[i].shape[1]
        part_ref[:, done : done + count, :] = earlier_refs[i][...]
        digit_ref[:, done : done + count, :] = earlier_refs[i + 1][...]
        done += count
    blocks = table_ref.shape[0] // BASE if turn else table_ref.shape[0]
    chunks = [(ref, at) for ref in arrived_refs for at in range(0, ref.shape[1], LANES)]
    pack = 2 if len(chunks) % 2 == 0 else 1
    width = pack * LANES
    half = depth // 2 if depth % 32 == 0 else depth
    low_of = lax.broadcasted_iota(jnp.int32, (BASE, width), 0).astype(jnp.float32)
    for first in range(0, len(chunks), pack):

        def read(rows):
            pieces = [ref[rows, at : at + LANES] for ref, at in chunks[first : first + pack]]
            return pieces[0] if pack == 1 else jnp.concatenate(pieces, axis=1)

        digits = read(slice(depth, depth + EXTRA)).astype(jnp.float32)
        low, high = digits[0:1], digits[1:2]
        lows = jnp.where(low_of == low, 1.0, 0.0).astype(jnp.bfloat16)
        dot = tsq = csq = jnp.zeros((1, width), jnp.float32)
        for top in range(0, depth, half):
            pieces = jnp.zeros((half, width), jnp.float32)
            for block in range(blocks):
                if turn and first == 0:
                    concepts = table_ref[block * BASE : (block + 1) * BASE, top : top + half].T
                    turned_ref[block, top : top + half, :] = concepts
                else:
                    source = turned_ref if turn else table_ref
                    concepts = source[block, top : top + half, :]
                found = jnp.dot(concepts, lows, preferred_element_type=jnp.float32)
                pieces = jnp.where(high == block + 1.0, found, pieces)
            floats = read(slice(top, top + half)).astype(jnp.float32)
            dot += jnp.sum(floats * pieces, axis=0, keepdims=True)
            tsq += jnp.sum(floats * floats, axis=0, keepdims=True)
            csq += jnp.sum(pieces * pieces, axis=0, keepdims=True)
        for step in range(pack):
            lane = slice(step * LANES, (step + 1) * LANES)
            b = done + first + step
            for q, sums in enumerate((dot, tsq, csq)):
                part_ref[q, b : b + 1, :] = sums[:, lane]
            digit_ref[0, b : b + 1, :] = low[:, lane]
            digit_ref[1, b : b + 1, :] = high[:, lane]


def match(arrived, table, depth, earlier):
    turn = table.ndim == 2
    blocks = table.shape[0] // BASE if turn else table.shape[0]
    count = sum(array.shape[1] for array in arrived) // LANES
    count += sum(pair[0].shape[1] for pair in earlier)
    operands = (*arrived, table, *(array for pair in earlier for array in pair))
    shapes = [
        jax.ShapeDtypeStruct((3, count, LANES), jnp.float32),
        jax.ShapeDtypeStruct((2, count, LANES), jnp.float32),
    ]
    if turn:
        shapes.append(jax.ShapeDtypeStruct((blocks, depth, BASE), jnp.bfloat16))
    part, digits, *turned = pl.pallas_call(
        functools.partial(match_kernel, len(arrived), depth, turn),
        out_shape=shapes,
        in_specs=[VMEM] * len(operands),
        out_specs=[VMEM] * len(shapes),
        compiler_params=GRANT,
        name="match",
    )(*operands)
    return part, digits, turned[0] if turn else table


def line(rows):
    return jnp.concatenate([rows[b : b + 1] for b in range(rows.shape[0])], axis=1)


def prepare_kernel(digit_ref, rank_ref, low_ref, turned_ref, top_ref, chosen_ref):
    low, high = line(digit_ref[0]), line(digit_ref[1])
    lows = lax.broadcasted_iota(jnp.int32, low_ref.shape, 0).astype(jnp.float32) == low
    low_ref[...] = jnp.where(lows, 1.0, 0.0).astype(jnp.bfloat16)
    turned_ref[...] = low_ref[...].T
    tops = lax.broadcasted_iota(jnp.int32, top_ref.shape, 0).astype(jnp.float32) + 1.0 == high
    top_ref[...] = jnp.where(tops, 1.0, 0.0)
    ranks = lax.broadcasted_iota(jnp.int32, chosen_ref.shape, 0).astype(jnp.float32)
    chosen_ref[...] = jnp.where(ranks == rank_ref[...], 1.0, 0.0).astype(jnp.bfloat16)


def join3(parts):
    rows = parts.shape[0] // 3
    return parts[:rows] + parts[rows : 2 * rows] + parts[2 * rows :]


def count_kernel(places, *refs):
    *part_refs, low_ref, turned_ref, top_ref, out_ref = refs
    sums = [ref[...] for ref in part_refs]
    while len(sums) > 1:
        sums = [sums[i] + sums[i + 1] for i in range(0, len(sums), 2)]
    dot, tsq, csq = sums[0][0], sums[0][1], sums[0][2]
    match = jax.nn.sigmoid(logit_scale * dot * lax.rsqrt(tsq + epsilon) * lax.rsqrt(csq + epsilon))
    capped = CAP * 1.0
    weights, tops = line(match), top_ref[...]
    spread = jnp.concatenate(split3(tops * weights), axis=0)
    count = join3(jnp.dot(spread, turned_ref[...], preferred_element_type=jnp.float32))
    parts = jnp.dot(jnp.concatenate(split3(count), axis=0), low_ref[...], preferred_element_type=jnp.float32)
    looked = jnp.sum(tops * join3(parts), axis=0, keepdims=True)
    balanced = weights * capped / jnp.maximum(looked, capped)
    blocks = match.shape[0]
    each = blocks // len(places) if places else 0
    for b in range(blocks):
        to = (lax.axis_index("dp") ^ places[b // each]) * each + b % each if places else b
        out_ref[pl.ds(to, 1), :] = balanced[:, b * LANES : (b + 1) * LANES]


def unslot_kernel(returned_ref, mark_ref, chosen_ref, out_ref):
    spread = jnp.concatenate(split3(returned_ref[...]), axis=0)
    found = join3(jnp.dot(spread, chosen_ref[...], preferred_element_type=jnp.float32))
    out_ref[...] = jnp.sum(mark_ref[...] * found, axis=0, keepdims=True)


def hops(groups):
    return tuple(step for step in ORDER if step < groups)


def chunks(groups):
    line = (0, *hops(groups))
    return tuple(zip(line[::2], line[1::2]))


def body(text, concept_table, ids):
    groups = lax.axis_size("dp")
    quarters = lax.axis_size("concept")
    pairs, depth = text.shape
    held = concept_table.shape[0]
    slots = 2 * pairs // groups
    total = groups * slots
    f32 = jnp.float32
    blocks = -(-held // BASE)
    wide = slots % LANES == 0 and groups in FEW

    table = jnp.pad(concept_table, ((0, blocks * BASE - held), (0, 0)))
    columns = slots if wide else total
    sheets = groups if wide else 1
    digits, partners, marks, rank = pl.pallas_call(
        functools.partial(rank_kernel, groups, held, wide),
        out_shape=(
            jax.ShapeDtypeStruct((EXTRA, pairs), f32),
            jax.ShapeDtypeStruct((groups, pairs), f32),
            jax.ShapeDtypeStruct((groups, pairs), f32),
            jax.ShapeDtypeStruct((1, pairs), f32),
        ),
        in_specs=[VMEM],
        out_specs=(VMEM,) * 4,
        compiler_params=GRANT,
        cost_estimate=pl.CostEstimate(flops=5 * 10**8, bytes_accessed=4 * pairs * groups, transcendentals=0),
        name="rank",
    )(ids.reshape(1, pairs))
    sent = pl.pallas_call(
        functools.partial(slot_kernel, groups, slots, wide),
        out_shape=[jax.ShapeDtypeStruct((depth + EXTRA, columns), jnp.bfloat16)] * sheets,
        in_specs=[VMEM] * 4,
        out_specs=[VMEM] * sheets,
        compiler_params=GRANT,
        cost_estimate=pl.CostEstimate(flops=10**9, bytes_accessed=4 * pairs * groups, transcendentals=0),
        name="slot",
    )(text, digits, partners, rank)
    if wide:
        arrived = {0: sent[0]}
        for step in hops(groups):
            arrived[step] = lax.ppermute(sent[step], "dp", [(i, i ^ step) for i in range(groups)])
        part = digits = None
        for chunk in chunks(groups):
            earlier = [] if part is None else [(part, digits)]
            part, digits, table = match([arrived[step] for step in chunk], table, depth, earlier)
        places = tuple(step for chunk in chunks(groups) for step in chunk)
    else:
        split = sent[0].reshape(depth + EXTRA, groups, slots).transpose(1, 0, 2)
        joined = lax.all_to_all(split, "dp", split_axis=0, concat_axis=0, tiled=True)
        joined = joined.transpose(1, 0, 2).reshape(depth + EXTRA, total)
        part, digits, table = match([joined], table, depth, [])
        places = None

    if quarters & (quarters - 1) == 0:
        parts = [part]
        for step in range(1, quarters):
            parts.append(lax.ppermute(part, "concept", [(i, i ^ step) for i in range(quarters)]))
    else:
        parts = [lax.psum(part, "concept")]

    highs = -(-blocks // 16) * 16
    tables = pl.pallas_call(
        prepare_kernel,
        out_shape=(
            jax.ShapeDtypeStruct((BASE, total), jnp.bfloat16),
            jax.ShapeDtypeStruct((total, BASE), jnp.bfloat16),
            jax.ShapeDtypeStruct((highs, total), f32),
            jax.ShapeDtypeStruct((slots, pairs), jnp.bfloat16),
        ),
        in_specs=[VMEM] * 2,
        out_specs=(VMEM,) * 4,
        compiler_params=GRANT,
        name="prepare",
    )(digits, rank)
    *tables, chosen = tables
    balanced = pl.pallas_call(
        functools.partial(count_kernel, places),
        out_shape=jax.ShapeDtypeStruct((total // LANES, LANES), f32),
        in_specs=[VMEM] * (len(parts) + 3),
        out_specs=VMEM,
        compiler_params=GRANT,
        name="count",
    )(*parts, *tables)

    returned = lax.all_to_all(balanced.reshape(groups, slots), "dp", split_axis=0, concat_axis=0, tiled=True)

    out = pl.pallas_call(
        unslot_kernel,
        out_shape=jax.ShapeDtypeStruct((1, pairs), f32),
        in_specs=[VMEM] * 3,
        out_specs=VMEM,
        compiler_params=GRANT,
        name="unslot",
    )(returned, marks, chosen)
    return out.reshape(pairs)


def solution(mesh):
    placed = (P("dp", "concept"), P("dp", "concept"), P("dp"))
    return jax.shard_map(body, mesh=mesh, in_specs=placed, out_specs=P("dp"), check_vma=False)
```

```python
import functools

import jax
import jax.numpy as jnp
from jax import lax
from jax.experimental import pallas as pl
from jax.experimental.pallas import tpu as pltpu
from jax.sharding import PartitionSpec as P


CAP = 16
BASE = 256
LANES = 128
EXTRA = 8
FEW = (4, 8)
ORDER = (6, 7, 2, 1, 4, 3, 5)


logit_scale = 64.0
epsilon = 1e-06

VMEM = pl.BlockSpec(memory_space=pltpu.VMEM)
GRANT = pltpu.CompilerParams(vmem_limit_bytes=16 * 1024 * 1024)


def split3(values):
    first = values.astype(jnp.bfloat16)
    rest = values - first.astype(jnp.float32)
    second = rest.astype(jnp.bfloat16)
    third = (rest - second.astype(jnp.float32)).astype(jnp.bfloat16)
    return first, second, third


def contract_lanes(left, right):
    return lax.dot_general(left, right, (((1,), (1,)), ((), ())), preferred_element_type=jnp.float32)


def rank_kernel(groups, held, wide, ids_ref, digit_ref, partner_ref, mark_ref, rank_ref):
    ids = ids_ref[...]
    pairs = ids.shape[1]
    me = lax.axis_index("dp") if wide else 0
    before = lax.broadcasted_iota(jnp.int32, (pairs, pairs), 0) < lax.broadcasted_iota(jnp.int32, (pairs, pairs), 1)
    triangle = jnp.where(before, 1.0, 0.0).astype(jnp.bfloat16)
    group = lax.broadcasted_iota(jnp.int32, (groups, pairs), 0)
    start = group * held
    marks = jnp.where((ids >= start) & (ids < start + held), 1.0, 0.0)
    partner = (group ^ me) * held
    partner_ref[...] = jnp.where((ids >= partner) & (ids < partner + held), 1.0, 0.0)
    seen = jnp.dot(marks.astype(jnp.bfloat16), triangle, preferred_element_type=jnp.float32)
    local = ids.astype(jnp.float32) - jnp.sum(marks * start.astype(jnp.float32), axis=0, keepdims=True)
    high = jnp.floor(local * (1.0 / BASE))
    row = lax.broadcasted_iota(jnp.int32, (EXTRA, pairs), 0)
    digit_ref[...] = jnp.where(row == 0, local - high * BASE, jnp.where(row == 1, high + 1.0, 0.0))
    mark_ref[...] = marks
    rank_ref[...] = jnp.sum(marks * seen, axis=0, keepdims=True)


def slot_kernel(groups, slots, wide, text_ref, digit_ref, partner_ref, rank_ref, *out_refs):
    pairs = text_ref.shape[0]
    marks, rank = partner_ref[...], rank_ref[...]
    if wide:
        ranks = lax.broadcasted_iota(jnp.int32, (slots, pairs), 0).astype(jnp.float32)
        ranked = jnp.where(ranks == rank, 1.0, 0.0).astype(jnp.bfloat16)
        marked = marks.astype(jnp.bfloat16)
        chosen = jnp.concatenate([ranked * marked[g : g + 1] for g in range(groups)], axis=0)
    else:
        group = lax.broadcasted_iota(jnp.int32, (groups, pairs), 0)
        target = jnp.sum(marks * (group * slots).astype(jnp.float32), axis=0, keepdims=True) + rank
        places = lax.broadcasted_iota(jnp.int32, (groups * slots, pairs), 0).astype(jnp.float32)
        chosen = jnp.where(places == target, 1.0, 0.0).astype(jnp.bfloat16)
    features = jnp.concatenate([text_ref[...].T, digit_ref[...].astype(jnp.bfloat16)], axis=0)
    moved = contract_lanes(features, chosen).astype(jnp.bfloat16)
    width = out_refs[0].shape[1]
    for g, out_ref in enumerate(out_refs):
        out_ref[...] = moved[:, g * width : (g + 1) * width]


def match_kernel(arrivals, depth, turn, *refs):
    if turn:
        *refs, turned_ref = refs
    *in_refs, part_ref, digit_ref = refs
    arrived_refs, table_ref, earlier_refs = in_refs[:arrivals], in_refs[arrivals], in_refs[arrivals + 1 :]
    done = 0
    for i in range(0, len(earlier_refs), 2):
        count = earlier_refs[i].shape[1]
        part_ref[:, done : done + count, :] = earlier_refs[i][...]
        digit_ref[:, done : done + count, :] = earlier_refs[i + 1][...]
        done += count
    blocks = table_ref.shape[0] // BASE if turn else table_ref.shape[0]
    chunks = [(ref, at) for ref in arrived_refs for at in range(0, ref.shape[1], LANES)]
    pack = 2 if len(chunks) % 2 == 0 else 1
    width = pack * LANES
    half = depth // 2 if depth % 32 == 0 else depth
    low_of = lax.broadcasted_iota(jnp.int32, (BASE, width), 0).astype(jnp.float32)
    for first in range(0, len(chunks), pack):

        def read(rows):
            pieces = [ref[rows, at : at + LANES] for ref, at in chunks[first : first + pack]]
            return pieces[0] if pack == 1 else jnp.concatenate(pieces, axis=1)

        digits = read(slice(depth, depth + EXTRA)).astype(jnp.float32)
        low, high = digits[0:1], digits[1:2]
        lows = jnp.where(low_of == low, 1.0, 0.0).astype(jnp.bfloat16)
        dot = tsq = csq = jnp.zeros((1, width), jnp.float32)
        for top in range(0, depth, half):
            pieces = jnp.zeros((half, width), jnp.float32)
            for block in range(blocks):
                if turn and first == 0:
                    concepts = table_ref[block * BASE : (block + 1) * BASE, top : top + half].T
                    turned_ref[block, top : top + half, :] = concepts
                else:
                    source = turned_ref if turn else table_ref
                    concepts = source[block, top : top + half, :]
                found = jnp.dot(concepts, lows, preferred_element_type=jnp.float32)
                pieces = jnp.where(high == block + 1.0, found, pieces)
            floats = read(slice(top, top + half)).astype(jnp.float32)
            dot += jnp.sum(floats * pieces, axis=0, keepdims=True)
            tsq += jnp.sum(floats * floats, axis=0, keepdims=True)
            csq += jnp.sum(pieces * pieces, axis=0, keepdims=True)
        for step in range(pack):
            lane = slice(step * LANES, (step + 1) * LANES)
            b = done + first + step
            for q, sums in enumerate((dot, tsq, csq)):
                part_ref[q, b : b + 1, :] = sums[:, lane]
            digit_ref[0, b : b + 1, :] = low[:, lane]
            digit_ref[1, b : b + 1, :] = high[:, lane]


def match(arrived, table, depth, earlier):
    turn = table.ndim == 2
    blocks = table.shape[0] // BASE if turn else table.shape[0]
    count = sum(array.shape[1] for array in arrived) // LANES
    count += sum(pair[0].shape[1] for pair in earlier)
    operands = (*arrived, table, *(array for pair in earlier for array in pair))
    shapes = [
        jax.ShapeDtypeStruct((3, count, LANES), jnp.float32),
        jax.ShapeDtypeStruct((2, count, LANES), jnp.float32),
    ]
    if turn:
        shapes.append(jax.ShapeDtypeStruct((blocks, depth, BASE), jnp.bfloat16))
    part, digits, *turned = pl.pallas_call(
        functools.partial(match_kernel, len(arrived), depth, turn),
        out_shape=shapes,
        in_specs=[VMEM] * len(operands),
        out_specs=[VMEM] * len(shapes),
        compiler_params=GRANT,
        name="match",
    )(*operands)
    return part, digits, turned[0] if turn else table


def line(rows):
    return jnp.concatenate([rows[b : b + 1] for b in range(rows.shape[0])], axis=1)


def prepare_kernel(digit_ref, rank_ref, low_ref, turned_ref, top_ref, chosen_ref):
    low, high = line(digit_ref[0]), line(digit_ref[1])
    lows = lax.broadcasted_iota(jnp.int32, low_ref.shape, 0).astype(jnp.float32) == low
    low_ref[...] = jnp.where(lows, 1.0, 0.0).astype(jnp.bfloat16)
    turned_ref[...] = low_ref[...].T
    tops = lax.broadcasted_iota(jnp.int32, top_ref.shape, 0).astype(jnp.float32) + 1.0 == high
    top_ref[...] = jnp.where(tops, 1.0, 0.0)
    ranks = lax.broadcasted_iota(jnp.int32, chosen_ref.shape, 0).astype(jnp.float32)
    chosen_ref[...] = jnp.where(ranks == rank_ref[...], 1.0, 0.0).astype(jnp.bfloat16)


def join3(parts):
    rows = parts.shape[0] // 3
    return parts[:rows] + parts[rows : 2 * rows] + parts[2 * rows :]


def count_kernel(places, *refs):
    *part_refs, low_ref, turned_ref, top_ref, out_ref = refs
    sums = [ref[...] for ref in part_refs]
    while len(sums) > 1:
        sums = [sums[i] + sums[i + 1] for i in range(0, len(sums), 2)]
    dot, tsq, csq = sums[0][0], sums[0][1], sums[0][2]
    match = jax.nn.sigmoid(logit_scale * dot * lax.rsqrt(tsq + epsilon) * lax.rsqrt(csq + epsilon))
    capped = CAP * 1.0
    weights, tops = line(match), top_ref[...]
    spread = jnp.concatenate(split3(tops * weights), axis=0)
    count = join3(jnp.dot(spread, turned_ref[...], preferred_element_type=jnp.float32))
    parts = jnp.dot(jnp.concatenate(split3(count), axis=0), low_ref[...], preferred_element_type=jnp.float32)
    looked = jnp.sum(tops * join3(parts), axis=0, keepdims=True)
    balanced = weights * capped / jnp.maximum(looked, capped)
    blocks = match.shape[0]
    each = blocks // len(places) if places else 0
    for b in range(blocks):
        to = (lax.axis_index("dp") ^ places[b // each]) * each + b % each if places else b
        out_ref[pl.ds(to, 1), :] = balanced[:, b * LANES : (b + 1) * LANES]


def unslot_kernel(returned_ref, mark_ref, chosen_ref, out_ref):
    spread = jnp.concatenate(split3(returned_ref[...]), axis=0)
    found = join3(jnp.dot(spread, chosen_ref[...], preferred_element_type=jnp.float32))
    out_ref[...] = jnp.sum(mark_ref[...] * found, axis=0, keepdims=True)


def hops(groups):
    return tuple(step for step in ORDER if step < groups)


def chunks(groups):
    line = (0, *hops(groups))
    middle = groups // 2
    return (line[:middle], *zip(line[middle::2], line[middle + 1 :: 2]))


def body(text, concept_table, ids):
    groups = lax.axis_size("dp")
    quarters = lax.axis_size("concept")
    pairs, depth = text.shape
    held = concept_table.shape[0]
    slots = 2 * pairs // groups
    total = groups * slots
    f32 = jnp.float32
    blocks = -(-held // BASE)
    wide = slots % LANES == 0 and groups in FEW

    table = jnp.pad(concept_table, ((0, blocks * BASE - held), (0, 0)))
    columns = slots if wide else total
    sheets = groups if wide else 1
    digits, partners, marks, rank = pl.pallas_call(
        functools.partial(rank_kernel, groups, held, wide),
        out_shape=(
            jax.ShapeDtypeStruct((EXTRA, pairs), f32),
            jax.ShapeDtypeStruct((groups, pairs), f32),
            jax.ShapeDtypeStruct((groups, pairs), f32),
            jax.ShapeDtypeStruct((1, pairs), f32),
        ),
        in_specs=[VMEM],
        out_specs=(VMEM,) * 4,
        compiler_params=GRANT,
        cost_estimate=pl.CostEstimate(flops=5 * 10**8, bytes_accessed=4 * pairs * groups, transcendentals=0),
        name="rank",
    )(ids.reshape(1, pairs))
    sent = pl.pallas_call(
        functools.partial(slot_kernel, groups, slots, wide),
        out_shape=[jax.ShapeDtypeStruct((depth + EXTRA, columns), jnp.bfloat16)] * sheets,
        in_specs=[VMEM] * 4,
        out_specs=[VMEM] * sheets,
        compiler_params=GRANT,
        cost_estimate=pl.CostEstimate(flops=10**9, bytes_accessed=4 * pairs * groups, transcendentals=0),
        name="slot",
    )(text, digits, partners, rank)
    if wide:
        arrived = {0: sent[0]}
        for step in hops(groups):
            arrived[step] = lax.ppermute(sent[step], "dp", [(i, i ^ step) for i in range(groups)])
        part = digits = None
        for chunk in chunks(groups):
            earlier = [] if part is None else [(part, digits)]
            part, digits, table = match([arrived[step] for step in chunk], table, depth, earlier)
        places = tuple(step for chunk in chunks(groups) for step in chunk)
    else:
        split = sent[0].reshape(depth + EXTRA, groups, slots).transpose(1, 0, 2)
        joined = lax.all_to_all(split, "dp", split_axis=0, concat_axis=0, tiled=True)
        joined = joined.transpose(1, 0, 2).reshape(depth + EXTRA, total)
        part, digits, table = match([joined], table, depth, [])
        places = None

    if quarters & (quarters - 1) == 0:
        parts = [part]
        for step in range(1, quarters):
            parts.append(lax.ppermute(part, "concept", [(i, i ^ step) for i in range(quarters)]))
    else:
        parts = [lax.psum(part, "concept")]

    highs = -(-blocks // 16) * 16
    tables = pl.pallas_call(
        prepare_kernel,
        out_shape=(
            jax.ShapeDtypeStruct((BASE, total), jnp.bfloat16),
            jax.ShapeDtypeStruct((total, BASE), jnp.bfloat16),
            jax.ShapeDtypeStruct((highs, total), f32),
            jax.ShapeDtypeStruct((slots, pairs), jnp.bfloat16),
        ),
        in_specs=[VMEM] * 2,
        out_specs=(VMEM,) * 4,
        compiler_params=GRANT,
        name="prepare",
    )(digits, rank)
    *tables, chosen = tables
    balanced = pl.pallas_call(
        functools.partial(count_kernel, places),
        out_shape=jax.ShapeDtypeStruct((total // LANES, LANES), f32),
        in_specs=[VMEM] * (len(parts) + 3),
        out_specs=VMEM,
        compiler_params=GRANT,
        name="count",
    )(*parts, *tables)

    returned = lax.all_to_all(balanced.reshape(groups, slots), "dp", split_axis=0, concat_axis=0, tiled=True)

    out = pl.pallas_call(
        unslot_kernel,
        out_shape=jax.ShapeDtypeStruct((1, pairs), f32),
        in_specs=[VMEM] * 3,
        out_specs=VMEM,
        compiler_params=GRANT,
        name="unslot",
    )(returned, marks, chosen)
    return out.reshape(pairs)


def solution(mesh):
    placed = (P("dp", "concept"), P("dp", "concept"), P("dp"))
    return jax.shard_map(body, mesh=mesh, in_specs=placed, out_specs=P("dp"), check_vma=False)
```
